32 devices in a mesh: ka: 4 (over y, x), ga: 8 (over z, core).
Axes of the slice: x: 2, y: 2, z: 4, core: 2. Of those that a mesh axis runs over, the one named last changes fastest.
Arguments:
- coeffs: bfloat16 [4, 1, 65536, 2, 512], P('ka', None, 'ga'), may hold values from -0.5 to 0.5
- counts: int32 [4, 1], replicated, may hold values from 32768 to 65536
- block_map: int32 [4, 1, 2048], replicated, may hold values from 0 to 2047, as said below
- wrap: int32 [4, 1, 2048], replicated, may hold values from 0 to 31
Outputs:
- margins: float32 [4, 512, 1, 2, 512], P('ka', 'ga')
The draws below stay inside these ranges and needn't reach their ends.
Inputs may be any that keep to these rules, and one draw needn't show every extreme that they name: For each k-point and line, block_map is a permutation of the 2048 blocks. Counting G-shards as runs of 256 blocks, at most 33 blocks of one shard have their partner blocks in any one shard, and for each k-point and line some pair of shards reaches 33.
All inputs are finite; a program needn't handle non-finite values.
Results may differ from the reference program's by a relative error of at most 0.0003.
Values may be sent and summed in bfloat16 or wider, within the bound.
No kernel may reach another device: no remote copies, remote signals or barrier semaphores. Data moves between devices by JAX's collectives and lax.ppermute only.
A program may use at most 128 MiB of HBM per device.

```python
import jax
import jax.numpy as jnp
from jax import lax

NB = 512
NPW = 65536
BLK = 32
LINES = 1
NK = 4
NBLK = 2048
BPD = 256
CAP = 33
N_GA = 8


def draw_block_map(key, part):
    shard_count = N_GA
    quarter = shard_count // 4
    line_keys = jax.random.split(jax.random.fold_in(key, 17), NK * LINES)

    def single_map(line_key):
        key_offsets, key_source, key_target = jax.random.split(line_key, 3)
        offsets = jax.random.permutation(key_offsets, shard_count)
        rank_ids = jnp.arange(shard_count, dtype=jnp.int32)
        level_mult = jnp.where(rank_ids < quarter, CAP, jnp.where(rank_ids < 2 * quarter, CAP - 2, CAP - 1)).astype(jnp.int32)
        multiplicity = jnp.zeros((shard_count,), jnp.int32).at[offsets].set(level_mult)
        cum_end = jnp.cumsum(multiplicity)
        slot_ids = jnp.arange(BPD, dtype=jnp.int32)
        offset_index = jnp.sum((slot_ids[:, None] >= cum_end[None, :]).astype(jnp.int32), axis=1)
        target_ids = jnp.arange(shard_count, dtype=jnp.int32)
        source_ids = (target_ids[:, None] + offset_index[None, :]) % shard_count
        source_perm = jax.vmap(lambda sub_key: jax.random.permutation(sub_key, BPD))(jax.random.split(key_source, shard_count)).astype(jnp.int32)
        target_perm = jax.vmap(lambda sub_key: jax.random.permutation(sub_key, BPD))(jax.random.split(key_target, shard_count)).astype(jnp.int32)
        values = source_ids * BPD + source_perm[source_ids, slot_ids[None, :]]
        write_at = target_ids[:, None] * BPD + target_perm
        return jnp.zeros((NBLK,), jnp.int32).at[write_at.reshape(-1)].set(values.reshape(-1).astype(jnp.int32))
    return jax.vmap(single_map)(line_keys).reshape(NK, LINES, NBLK).astype(jnp.int32)


def touch_ends(array, own_key, low, top_value):
    spot = [jax.random.randint(jax.random.fold_in(own_key, axis), (), 0, length) for axis, length in enumerate(array.shape)]
    longest = array.shape.index(max(array.shape))
    next_to = spot[:longest] + [(spot[longest] + 1) % array.shape[longest]] + spot[longest + 1:]
    return array.at[tuple(spot)].set(low).at[tuple(next_to)].set(top_value)


def shard_levels(rng, dims, pieces, least, top_value):
    def one(axis_at, shards_of):
        draws = jax.random.uniform(jax.random.fold_in(jax.random.fold_in(rng, 6), axis_at), (shards_of,), jnp.float32, least / len(pieces), top_value / len(pieces))
        return jnp.repeat(jnp.exp(draws), dims[axis_at] // shards_of).reshape((-1,) + (1,) * (len(dims) - axis_at - 1))

    loudness = one(*pieces[0])
    for cut in pieces[1:]:
        loudness = loudness * one(*cut)
    return loudness


def centred(rng, extent, width, bound, shards=(), held_as=jnp.bfloat16):
    gain = shard_levels(rng, extent, shards, -0.22, 0.18) if shards else 1.0
    entries = jax.random.normal(rng, extent, jnp.float32) * width * gain
    return jnp.minimum(jnp.maximum(entries, -bound), bound).astype(held_as)


def setup_inputs(seed: int = 0) -> dict:
    arg_keys = jax.random.split(jax.random.key(seed), 5)
    coeffs = centred(arg_keys[0], (NK, LINES, NPW, 2, NB), 0.0625, 0.5, ((0, 4), (2, 8)))
    counts = touch_ends(jax.random.randint(arg_keys[1], (NK, LINES), NPW // 2, NPW + 1), jax.random.fold_in(arg_keys[1], 1), NPW // 2, NPW).astype(jnp.int32)
    block_map = draw_block_map(jax.random.fold_in(arg_keys[4], 71), 0)
    wrap = touch_ends(jax.random.randint(arg_keys[3], (NK, LINES, NBLK), 0, BLK), jax.random.fold_in(arg_keys[3], 1), 0, BLK - 1).astype(jnp.int32)
    return dict(coeffs=coeffs, counts=counts, block_map=block_map, wrap=wrap)


def reference(coeffs, counts, block_map, wrap):
    g_ids = jnp.arange(NPW, dtype=jnp.int32)
    blk_ids = g_ids // BLK
    lane_ids = g_ids % BLK

    def margin_at(k_here):
        k_next = (k_here + 1) % NK
        per_line = []
        for line_idx in range(LINES):
            block_src = block_map[k_here, line_idx]
            wrap_src = wrap[k_here, line_idx]
            src_rows = (block_src[blk_ids] * BLK + (lane_ids + wrap_src[blk_ids]) % BLK).astype(jnp.int32)
            usable = (g_ids < counts[k_here, line_idx]) & (src_rows < counts[k_next, line_idx])
            left_side = jnp.where(usable[:, None, None], coeffs[k_here, line_idx].astype(jnp.float32), jnp.zeros((), jnp.float32))
            right_side = coeffs[k_next, line_idx][src_rows].astype(jnp.float32)
            products = jnp.einsum("gcm,gdn->mcdn", left_side, right_side, precision=lax.Precision.HIGHEST)
            real_part = products[:, 0, 0] + products[:, 1, 1]
            imag_part = products[:, 0, 1] - products[:, 1, 0]
            per_line.append(jnp.stack([real_part, imag_part], axis=1))
        return jnp.stack(per_line, axis=1)

    return lax.map(margin_at, jnp.arange(NK, dtype=jnp.int32))
```

```python
import functools

import jax
import jax.numpy as jnp
from jax import lax
from jax.experimental import pallas as pl
from jax.experimental.pallas import tpu as pltpu
from jax.sharding import PartitionSpec as P

BLK = 32


def chunk_bounds(capacity):
    pieces = 3 if capacity >= 3 else 1
    return [(capacity * i // pieces, capacity * (i + 1) // pieces) for i in range(pieces)]


def pack_kernel(first, capacity, group, rotate, table, *refs):
    ins, out = refs[:group], refs[group]
    slots = table.shape[0] // 4
    rank = first + pl.program_id(0)
    for d in range(group):
        entry = (pl.program_id(1) * group + d) * capacity + rank
        if not rotate:
            out[d, 0] = ins[d][...]
            continue
        shift = table[slots + entry]
        left_end = table[2 * slots + entry]
        right_end = table[3 * slots + entry]
        for p in range(BLK):
            lane = (p - shift) & (BLK - 1)
            row = ins[d][lane]
            live = (lane < left_end) & (p < right_end)
            out[d, 0, p] = jnp.where(live, row, jnp.zeros_like(row))


def pack(source, table, bounds, capacity, shards, rotate):
    first, last = bounds
    group = min(8, shards)
    _, _, bands = source.shape
    ranks = last - first

    def picked(d):
        return lambda r, s, table: (table[(s * group + d) * capacity + first + r], 0, 0)

    moved = shards * ranks * BLK * 2 * bands * 2
    return pl.pallas_call(
        functools.partial(pack_kernel, first, capacity, group, rotate),
        grid_spec=pltpu.PrefetchScalarGridSpec(
            num_scalar_prefetch=1,
            grid=(ranks, shards // group),
            in_specs=[pl.BlockSpec((BLK, 2, bands), picked(d)) for d in range(group)],
            out_specs=pl.BlockSpec((group, 1, BLK, 2, bands), lambda r, s, table: (s, r, 0, 0, 0)),
        ),
        out_shape=jax.ShapeDtypeStruct((shards, ranks, BLK, 2, bands), source.dtype),
        cost_estimate=pl.CostEstimate(flops=4 * moved, bytes_accessed=2 * moved, transcendentals=0),
        name="pack_left" if rotate else "pack_right",
    )(table, *([source] * group))


def local(coeffs, counts, block_map, wrap):
    held = coeffs[0]
    lines, g_rows, _, bands = held.shape
    shards = lax.axis_size("ga")
    per_shard = g_rows // BLK
    blocks = block_map.shape[-1]
    capacity = blocks // (shards * shards) + 1
    k_total = counts.shape[0]
    k = lax.axis_index("ka")
    g = lax.axis_index("ga")
    k_next = (k + 1) % k_total
    k_prev = (k + k_total - 1) % k_total
    ids = jnp.arange(per_shard, dtype=jnp.int32)
    slot_ids = jnp.arange(capacity, dtype=jnp.int32)
    shard_ids = jnp.arange(shards, dtype=jnp.int32)
    down = [(s, (s - 1) % k_total) for s in range(k_total)]
    rows_here = bands // shards
    outs = []
    for line in range(lines):
        mine = lax.dynamic_slice_in_dim(block_map[k, line], g * per_shard, per_shard, 0)
        shift = lax.dynamic_slice_in_dim(wrap[k, line], g * per_shard, per_shard, 0)
        target = mine // per_shard
        rank = jnp.sum(
            ((target[:, None] == target[None, :]) & (ids[:, None] > ids[None, :])).astype(jnp.int32), axis=1
        )
        left_end = counts[k, line] - (g * g_rows + ids * BLK)
        right_end = counts[k_next, line] - mine * BLK
        hit = (target[None, None, :] == shard_ids[:, None, None]) & (rank[None, None, :] == slot_ids[None, :, None])
        values = jnp.stack([ids, shift, left_end, right_end])
        left_table = jnp.sum(jnp.where(hit[None], values[:, None, None, :], 0), axis=3).reshape(-1)
        theirs = block_map[k_prev, line].reshape(shards, per_shard)
        for_me = theirs // per_shard == g
        rank_in = jnp.sum((for_me[:, None, :] & (ids[:, None] > ids[None, :])[None]).astype(jnp.int32), axis=2)
        hit_in = for_me[:, None, :] & (rank_in[:, None, :] == slot_ids[None, :, None])
        right_table = jnp.sum(jnp.where(hit_in, (theirs % per_shard)[:, None, :], 0), axis=2).reshape(-1)
        right_table = jnp.concatenate([right_table] * 4)

        rows = held[line]
        total = None
        for bounds in chunk_bounds(capacity):
            sent = pack(rows, left_table, bounds, capacity, shards, True)
            left = lax.all_to_all(sent, "ga", split_axis=0, concat_axis=0, tiled=True)
            right = pack(rows, right_table, bounds, capacity, shards, False)
            right = lax.ppermute(right, "ka", down)
            count = shards * (bounds[1] - bounds[0]) * BLK
            products = jnp.einsum(
                "gcm,gdn->mcdn",
                left.reshape(count, 2, bands),
                right.reshape(count, 2, bands),
                preferred_element_type=jnp.float32,
            )
            part = jnp.stack(
                [products[:, 0, 0] + products[:, 1, 1], products[:, 0, 1] - products[:, 1, 0]], axis=1
            )
            total = part if total is None else total + part
        outs.append(lax.psum_scatter(total, "ga", scatter_dimension=0, tiled=True))
    return jnp.stack(outs, axis=1)[None]


def solution(mesh):
    placed = (P("ka", None, "ga", None, None), P(), P(), P())
    return jax.shard_map(
        local,
        mesh=mesh,
        in_specs=placed,
        out_specs=P("ka", "ga", None, None, None),
        check_vma=False,
    )
```

```python
import functools

import jax
import jax.numpy as jnp
from jax import lax
from jax.experimental import pallas as pl
from jax.experimental.pallas import tpu as pltpu
from jax.sharding import PartitionSpec as P


BLK = 32


def offset_order(shards):
    far = sorted(range(1, shards), key=lambda d: (abs(d - shards // 2), d))
    return far[:1] + [0] + far[1:]


def chunks(shards):
    order = offset_order(shards)
    width = max(1, shards // 8)
    return [order[i : i + width] for i in range(0, shards, width)]


def pack_kernel(offset, group, capacity, shards, rotate, table, place, *refs):
    ins, out = refs[:group], refs[group]
    slots = shards * capacity
    row = lax.rem(place[0] + offset + shards, shards)
    entry = row * capacity + pl.program_id(0) * group
    if not rotate:
        for d in range(group):
            out[d] = ins[d][...]
        return
    shifts = [table[slots + entry + d] for d in range(group)]
    left_ends = [table[2 * slots + entry + d] for d in range(group)]
    right_ends = [table[3 * slots + entry + d] for d in range(group)]

    @pl.loop(0, BLK, unroll=2)
    def _(p):
        for d in range(group):
            lane = (p - shifts[d]) & (BLK - 1)
            values = ins[d][lane]
            live = (lane < left_ends[d]) & (p < right_ends[d])
            out[d, p] = jnp.where(live, values, jnp.zeros_like(values))


def pack(source, table, place, offset, capacity, shards, rotate):
    bands = source.shape[-1]
    group = max(n for n in range(1, 12) if capacity % n == 0)

    def picked(d):
        def index(step, table, place):
            row = lax.rem(place[0] + offset + shards, shards)
            return table[row * capacity + step * group + d], 0, 0

        return index

    moved = capacity * BLK * 2 * bands * 2
    return pl.pallas_call(
        functools.partial(pack_kernel, offset, group, capacity, shards, rotate),
        grid_spec=pltpu.PrefetchScalarGridSpec(
            num_scalar_prefetch=2,
            grid=(capacity // group,),
            in_specs=[pl.BlockSpec((BLK, 2, bands), picked(d)) for d in range(group)],
            out_specs=pl.BlockSpec((group, BLK, 2, bands), lambda step, table, place: (step, 0, 0, 0)),
        ),
        out_shape=jax.ShapeDtypeStruct((capacity, BLK, 2, bands), source.dtype),
        cost_estimate=pl.CostEstimate(flops=4 * moved, bytes_accessed=2 * moved, transcendentals=0),
        name="pack_left" if rotate else "pack_right",
    )(table, place, *([source] * group))


def scatter_sum(total, shards):
    core = lax.axis_index("ga") % 2
    chip = lax.axis_index("ga") // 2
    chips = shards // 2
    pairs = total.reshape(chips, 2, *total.shape[1:])
    swap = [(s, s ^ 1) for s in range(shards)]
    theirs = lax.dynamic_index_in_dim(pairs, 1 - core, 1, keepdims=False)
    ours = lax.dynamic_index_in_dim(pairs, core, 1, keepdims=False)
    ours = ours + lax.ppermute(theirs, "ga", swap)
    result = lax.dynamic_index_in_dim(ours, chip, 0, keepdims=False)
    for step in range(1, chips):
        part = lax.dynamic_index_in_dim(ours, (chip + step) % chips, 0, keepdims=False)
        result = result + lax.ppermute(part, "ga", [(s, (s + 2 * step) % shards) for s in range(shards)])
    return result


def local(coeffs, counts, block_map, wrap):
    held = coeffs[0]
    lines, g_rows, _, bands = held.shape
    shards = lax.axis_size("ga")
    per_shard = g_rows // BLK
    blocks = block_map.shape[-1]
    capacity = blocks // (shards * shards) + 1
    k_total = counts.shape[0]
    k = lax.axis_index("ka")
    g = lax.axis_index("ga")
    k_next = (k + 1) % k_total
    k_prev = (k + k_total - 1) % k_total
    ids = jnp.arange(per_shard, dtype=jnp.int32)
    slot_ids = jnp.arange(capacity, dtype=jnp.int32)
    shard_ids = jnp.arange(shards, dtype=jnp.int32)
    place = g.astype(jnp.int32).reshape(1)
    down = [(s, (s - 1) % k_total) for s in range(k_total)]
    rows_here = bands // shards
    outs = []
    for line in range(lines):
        mine = lax.dynamic_slice_in_dim(block_map[k, line], g * per_shard, per_shard, 0)
        shift = lax.dynamic_slice_in_dim(wrap[k, line], g * per_shard, per_shard, 0)
        target = mine // per_shard
        rank = jnp.sum(
            ((target[:, None] == target[None, :]) & (ids[:, None] > ids[None, :])).astype(jnp.int32), axis=1
        )
        left_end = counts[k, line] - (g * g_rows + ids * BLK)
        right_end = counts[k_next, line] - mine * BLK
        hit = (target[None, None, :] == shard_ids[:, None, None]) & (rank[None, None, :] == slot_ids[None, :, None])
        values = jnp.stack([ids, shift, left_end, right_end])
        left_table = jnp.sum(jnp.where(hit[None], values[:, None, None, :], 0), axis=3).reshape(-1)
        theirs = block_map[k_prev, line].reshape(shards, per_shard)
        for_me = theirs // per_shard == g
        rank_in = jnp.sum((for_me[:, None, :] & (ids[:, None] > ids[None, :])[None]).astype(jnp.int32), axis=2)
        hit_in = for_me[:, None, :] & (rank_in[:, None, :] == slot_ids[None, :, None])
        right_table = jnp.sum(jnp.where(hit_in, (theirs % per_shard)[:, None, :], 0), axis=2).reshape(-1)

        rows = held[line]
        total = None
        for together in chunks(shards):
            lefts, rights = [], []
            for d in together:
                left = pack(rows, left_table, place, d, capacity, shards, True)
                left_table, right_table, left = lax.optimization_barrier((left_table, right_table, left))
                if d:
                    left = lax.ppermute(left, "ga", [(s, (s + d) % shards) for s in range(shards)])
                right = pack(rows, right_table, place, -d, capacity, shards, False)
                left_table, right_table, right = lax.optimization_barrier((left_table, right_table, right))
                right = lax.ppermute(right, "ka", down)
                lefts.append(left)
                rights.append(right)
            left = lefts[0] if len(lefts) == 1 else jnp.concatenate(lefts)
            right = rights[0] if len(rights) == 1 else jnp.concatenate(rights)
            count = len(together) * capacity * BLK
            products = jnp.einsum(
                "gcm,gdn->mcdn",
                left.reshape(count, 2, bands),
                right.reshape(count, 2, bands),
                preferred_element_type=jnp.float32,
            )
            part = jnp.stack(
                [products[:, 0, 0] + products[:, 1, 1], products[:, 0, 1] - products[:, 1, 0]], axis=1
            )
            total = part if total is None else total + part
        outs.append(scatter_sum(total.reshape(shards, rows_here, 2, bands), shards))
    return jnp.stack(outs, axis=1)[None]


def solution(mesh):
    placed = (P("ka", None, "ga", None, None), P(), P(), P())

    return jax.shard_map(
        local,
        mesh=mesh,
        in_specs=placed,
        out_specs=P("ka", "ga", None, None, None),
        check_vma=False,
    )
```

```python
import functools

import jax
import jax.numpy as jnp
from jax import lax
from jax.experimental import pallas as pl
from jax.experimental.pallas import tpu as pltpu
from jax.sharding import PartitionSpec as P


BLK = 32


def offset_order(shards):
    far = sorted(range(1, shards), key=lambda d: (abs(d - shards // 2), d))
    return far[:1] + [0] + far[1:]


def chunks(shards):
    order = offset_order(shards)
    width = max(1, shards // 8)
    return [order[i : i + width] for i in range(0, shards, width)]


def pack_kernel(offset, group, capacity, shards, rotate, table, place, *refs):
    ins, out = refs[:group], refs[group]
    slots = shards * capacity
    row = lax.rem(place[0] + offset + shards, shards)
    entry = row * capacity + pl.program_id(0) * group
    if not rotate:
        for d in range(group):
            out[d] = ins[d][...]
        return
    shifts = [table[slots + entry + d] for d in range(group)]
    left_ends = [table[2 * slots + entry + d] for d in range(group)]
    right_ends = [table[3 * slots + entry + d] for d in range(group)]

    @pl.loop(0, BLK, unroll=2)
    def _(p):
        for d in range(group):
            lane = (p - shifts[d]) & (BLK - 1)
            values = ins[d][lane]
            live = (lane < left_ends[d]) & (p < right_ends[d])
            out[d, p] = jnp.where(live, values, jnp.zeros_like(values))


def pack(source, table, place, offset, capacity, shards, rotate):
    bands = source.shape[-1]
    group = max(n for n in range(1, 12) if capacity % n == 0)

    def picked(d):
        def index(step, table, place):
            row = lax.rem(place[0] + offset + shards, shards)
            return table[row * capacity + step * group + d], 0, 0

        return index

    moved = capacity * BLK * 2 * bands * 2
    return pl.pallas_call(
        functools.partial(pack_kernel, offset, group, capacity, shards, rotate),
        grid_spec=pltpu.PrefetchScalarGridSpec(
            num_scalar_prefetch=2,
            grid=(capacity // group,),
            in_specs=[pl.BlockSpec((BLK, 2, bands), picked(d)) for d in range(group)],
            out_specs=pl.BlockSpec((group, BLK, 2, bands), lambda step, table, place: (step, 0, 0, 0)),
        ),
        out_shape=jax.ShapeDtypeStruct((capacity, BLK, 2, bands), source.dtype),
        cost_estimate=pl.CostEstimate(flops=4 * moved, bytes_accessed=2 * moved, transcendentals=0),
        name="pack_left" if rotate else "pack_right",
    )(table, place, *([source] * group))


def scatter_sum(total, shards):
    place = lax.axis_index("ga")
    span = 1
    while shards % (2 * span) == 0 and span < shards:
        bit = (place // span) % 2
        pairs = total.reshape(-1, 2, *total.shape[1:])
        theirs = lax.dynamic_index_in_dim(pairs, 1 - bit, 1, keepdims=False)
        ours = lax.dynamic_index_in_dim(pairs, bit, 1, keepdims=False)
        total = ours + lax.ppermute(theirs, "ga", [(s, s ^ span) for s in range(shards)])
        span *= 2
    if span == shards:
        return total[0]
    place = place // span
    rest = shards // span
    result = lax.dynamic_index_in_dim(total, place, 0, keepdims=False)
    for step in range(1, rest):
        part = lax.dynamic_index_in_dim(total, (place + step) % rest, 0, keepdims=False)
        result = result + lax.ppermute(part, "ga", [(s, (s + span * step) % shards) for s in range(shards)])
    return result


def local(coeffs, counts, block_map, wrap):
    held = coeffs[0]
    lines, g_rows, _, bands = held.shape
    shards = lax.axis_size("ga")
    per_shard = g_rows // BLK
    blocks = block_map.shape[-1]
    capacity = blocks // (shards * shards) + 1
    k_total = counts.shape[0]
    k = lax.axis_index("ka")
    g = lax.axis_index("ga")
    k_next = (k + 1) % k_total
    k_prev = (k + k_total - 1) % k_total
    ids = jnp.arange(per_shard, dtype=jnp.int32)
    slot_ids = jnp.arange(capacity, dtype=jnp.int32)
    shard_ids = jnp.arange(shards, dtype=jnp.int32)
    place = g.astype(jnp.int32).reshape(1)
    down = [(s, (s - 1) % k_total) for s in range(k_total)]
    rows_here = bands // shards
    outs = []
    for line in range(lines):
        mine = lax.dynamic_slice_in_dim(block_map[k, line], g * per_shard, per_shard, 0)
        shift = lax.dynamic_slice_in_dim(wrap[k, line], g * per_shard, per_shard, 0)
        target = mine // per_shard
        rank = jnp.sum(
            ((target[:, None] == target[None, :]) & (ids[:, None] > ids[None, :])).astype(jnp.int32), axis=1
        )
        left_end = counts[k, line] - (g * g_rows + ids * BLK)
        right_end = counts[k_next, line] - mine * BLK
        hit = (target[None, None, :] == shard_ids[:, None, None]) & (rank[None, None, :] == slot_ids[None, :, None])
        values = jnp.stack([ids, shift, left_end, right_end])
        left_table = jnp.sum(jnp.where(hit[None], values[:, None, None, :], 0), axis=3).reshape(-1)
        theirs = block_map[k_prev, line].reshape(shards, per_shard)
        for_me = theirs // per_shard == g
        rank_in = jnp.sum((for_me[:, None, :] & (ids[:, None] > ids[None, :])[None]).astype(jnp.int32), axis=2)
        hit_in = for_me[:, None, :] & (rank_in[:, None, :] == slot_ids[None, :, None])
        right_table = jnp.sum(jnp.where(hit_in, (theirs % per_shard)[:, None, :], 0), axis=2).reshape(-1)

        rows = held[line]
        total = None
        for together in chunks(shards):
            lefts, rights = [], []
            for d in together:
                right = pack(rows, right_table, place, -d, capacity, shards, False)
                left_table, right_table, right = lax.optimization_barrier((left_table, right_table, right))
                right = lax.ppermute(right, "ka", down)
                left = pack(rows, left_table, place, d, capacity, shards, True)
                left_table, right_table, left = lax.optimization_barrier((left_table, right_table, left))
                if d:
                    left = lax.ppermute(left, "ga", [(s, (s + d) % shards) for s in range(shards)])
                lefts.append(left)
                rights.append(right)
            left = lefts[0] if len(lefts) == 1 else jnp.concatenate(lefts)
            right = rights[0] if len(rights) == 1 else jnp.concatenate(rights)
            count = len(together) * capacity * BLK
            products = jnp.einsum(
                "gcm,gdn->mcdn",
                left.reshape(count, 2, bands),
                right.reshape(count, 2, bands),
                preferred_element_type=jnp.float32,
            )
            part = jnp.stack(
                [products[:, 0, 0] + products[:, 1, 1], products[:, 0, 1] - products[:, 1, 0]], axis=1
            )
            total = part if total is None else total + part
        outs.append(scatter_sum(total.reshape(shards, rows_here, 2, bands), shards))
    return jnp.stack(outs, axis=1)[None]


def solution(mesh):
    placed = (P("ka", None, "ga", None, None), P(), P(), P())

    return jax.shard_map(
        local,
        mesh=mesh,
        in_specs=placed,
        out_specs=P("ka", "ga", None, None, None),
        check_vma=False,
    )
```

```python
import functools

import jax
import jax.numpy as jnp
from jax import lax
from jax.experimental import pallas as pl
from jax.experimental.pallas import tpu as pltpu
from jax.sharding import PartitionSpec as P


BLK = 32
TOGETHER = 2
OVER_ROWS = (((0,), (0,)), ((), ()))


def unit_of(count):
    return max(n for n in range(1, 12) if count % n == 0)


def pieces_of(shards, capacity):
    middle = shards // 2
    late = sorted({2 % shards, -2 % shards}) if shards >= 8 else []
    rest = sorted(set(range(1, shards)) - {middle} - set(late), key=lambda d: (abs(d - middle), d))
    heads = sorted({0, -(-capacity // 6), -(-capacity // 2), capacity})
    tail = capacity - -(-capacity // 6) if capacity > 1 else 0
    pieces = [(middle, first, end) for first, end in zip(heads[:-1], heads[1:])]
    pieces += [(d, 0, capacity) for d in [0] + rest]
    if tail:
        pieces += [(d, 0, tail) for d in late]
    return pieces + [(d, tail, capacity) for d in late]


def groups_of(pieces):
    ends = [list(pieces[-4:-2]), list(pieces[-2:])]
    front = list(pieces[:-4])
    head, front = front[:4], front[4:]
    first, front = front[:1], front[1:]
    return [g for g in [head, first] + [front[i : i + 3] for i in range(0, len(front), 3)] + ends if g]


def pack_kernel(jobs, unit, capacity, shards, blocks, line, table, place, counts, *refs):
    ins, outs = refs[: unit * len(jobs)], refs[unit * len(jobs) :]
    per_shard = blocks // shards
    k = lax.axis_index("ka")
    count_here = counts[line, k]
    count_next = counts[line, lax.rem(k + 1, counts.shape[1])]
    for at, ((offset, first, _), rotate) in enumerate(jobs):
        sources, out = ins[at * unit : (at + 1) * unit], outs[at]
        if not rotate:
            for d in range(unit):
                out[d] = sources[d][...]
            continue
        row = lax.rem(place[0] + offset + shards, shards)
        entry = row * capacity + first + pl.program_id(0) * unit
        shifts, left_ends, right_ends = [], [], []
        for d in range(unit):
            code = table[entry + d]
            own = place[0] * per_shard + lax.rem(code, per_shard)
            rest = lax.div(code, per_shard)
            partner = lax.div(rest, BLK)
            shifts.append(lax.rem(rest, BLK))
            left_ends.append(count_here - own * BLK)
            right_ends.append(jnp.where(partner == 0, 0, count_next - (partner - 1) * BLK))

        @pl.loop(0, BLK, unroll=2)
        def _(p):
            for d in range(unit):
                lane = (p - shifts[d]) & (BLK - 1)
                values = sources[d][lane]
                live = (lane < left_ends[d]) & (p < right_ends[d])
                out[d, p] = jnp.where(live, values, jnp.zeros_like(values))


def pack(source, table, place, counts, jobs, capacity, shards, blocks, line):
    bands = source.shape[-1]
    count = jobs[0][0][2] - jobs[0][0][1]
    unit = unit_of(count)

    def picked(job, d):
        (offset, first, _), rotate = job
        base = 0 if rotate else shards

        def index(step, table, place, counts):
            row = lax.rem(place[0] + offset + shards, shards)
            code = table[(row + base) * capacity + first + step * unit + d]
            return lax.rem(code, blocks // shards), 0, 0

        return index

    moved = count * BLK * 2 * bands * 2 * len(jobs)
    return pl.pallas_call(
        functools.partial(pack_kernel, jobs, unit, capacity, shards, blocks, line),
        grid_spec=pltpu.PrefetchScalarGridSpec(
            num_scalar_prefetch=3,
            grid=(count // unit,),
            in_specs=[pl.BlockSpec((BLK, 2, bands), picked(job, d)) for job in jobs for d in range(unit)],
            out_specs=[pl.BlockSpec((unit, BLK, 2, bands), lambda step, table, place, counts: (step, 0, 0, 0))]
            * len(jobs),
        ),
        out_shape=[jax.ShapeDtypeStruct((count, BLK, 2, bands), source.dtype)] * len(jobs),
        cost_estimate=pl.CostEstimate(flops=4 * moved, bytes_accessed=2 * moved, transcendentals=0),
        name="pack",
    )(table, place, counts, *([source] * (unit * len(jobs))))


def product_kernel(starts, carried, split, *refs):
    n = len(starts)
    sums = refs[2 * n + carried :]
    step = pl.program_id(0)
    core = lax.rem(lax.axis_index("ga"), 2)

    @pl.when(step == 0)
    def _():
        if not split:
            sums[0][...] = refs[2 * n][...] if carried else jnp.zeros_like(sums[0])
            return
        for part in range(2):
            for chip in range(sums[0].shape[0]):
                if carried:
                    sums[part][chip] = refs[2 * n][part, 2 * chip + 1 - core]
                    sums[2 + part][chip] = refs[2 * n][part, 2 * chip + core]
                else:
                    sums[part][chip] = jnp.zeros_like(sums[part][chip])
                    sums[2 + part][chip] = jnp.zeros_like(sums[part][chip])

    def rows_of(held):
        panels = [ref[...].reshape(ref.shape[0] * BLK * 2, ref.shape[-1]) for ref in held]
        return panels[0] if len(panels) == 1 else jnp.concatenate(panels)

    for i, (begin, end) in enumerate(starts[:1] if split else starts):

        @pl.when((step >= begin) & (step < end))
        def _():
            left = rows_of(refs[:n] if split else refs[i : i + 1])
            right = rows_of(refs[n : 2 * n] if split else refs[n + i : n + i + 1])
            depth = right.shape[0]
            odd = lax.broadcasted_iota(jnp.int32, right.shape, 0) % 2 == 1
            turned = jnp.where(odd, -pltpu.roll(right, 1, 0), pltpu.roll(right, depth - 1, 0))
            for part, factor in enumerate((right, turned)):
                added = lax.dot_general(left, factor, OVER_ROWS, preferred_element_type=jnp.float32)
                if not split:
                    sums[0][part] += added
                    continue
                halves = added.reshape(sums[0].shape[0], 2, *sums[0].shape[1:])
                sums[part][...] += jnp.where(core == 0, halves[:, 1], halves[:, 0])
                sums[2 + part][...] += jnp.where(core == 0, halves[:, 0], halves[:, 1])


def product(lefts, rights, total, shards, split):
    bands = lefts[0].shape[-1]
    starts, steps = [], 0
    for piece in lefts:
        starts.append((steps, steps + piece.shape[0] // unit_of(piece.shape[0])))
        steps = starts[-1][1]
    if split:
        starts, steps = [(0, 1)] * len(lefts), 1

    def panel(piece, begin, end):
        return pl.BlockSpec(
            (piece.shape[0] // (end - begin), BLK, 2, bands),
            lambda step: (jnp.clip(step - begin, 0, end - begin - 1), 0, 0, 0),
        )

    panels = [panel(piece, *ends) for piece, ends in zip(lefts, starts)]
    sums = pl.BlockSpec((2, bands, bands), lambda step: (0, 0, 0))
    carried = [] if total is None else [total]
    if carried and split:
        carried = [total.reshape(2, shards, bands // shards, bands)]
    rows = sum(piece.shape[0] for piece in lefts) * BLK
    half = (shards // 2, bands // shards, bands)
    return pl.pallas_call(
        functools.partial(product_kernel, starts, len(carried), split),
        grid=(steps,),
        in_specs=panels
        + panels
        + [pl.BlockSpec(total.shape, lambda step, rank=total.ndim: (0,) * rank) for total in carried],
        out_specs=[pl.BlockSpec(half, lambda step: (0, 0, 0))] * 4 if split else sums,
        out_shape=[jax.ShapeDtypeStruct(half, jnp.float32)] * 4
        if split
        else jax.ShapeDtypeStruct((2, bands, bands), jnp.float32),
        input_output_aliases={2 * len(lefts): 0} if carried and not split else {},
        cost_estimate=pl.CostEstimate(
            flops=8 * rows * bands * bands, bytes_accessed=8 * rows * bands, transcendentals=0
        ),
        compiler_params=pltpu.CompilerParams(vmem_limit_bytes=25165824 if split else 67043328),
        name="product",
    )(*lefts, *rights, *carried)


def scatter_sum(theirs, ours, shards):
    place = lax.axis_index("ga")
    swap = [(s, s ^ 1) for s in range(shards)]
    terms = [(mine, lax.ppermute(other, "ga", swap)) for mine, other in zip(ours, theirs)]
    span = 2
    while shards % (2 * span) == 0 and span < shards:
        bit = (place // span) % 2
        swap = [(s, s ^ span) for s in range(shards)]
        for at, pair in enumerate(terms):
            split = [term.reshape(-1, 2, *term.shape[1:]) for term in pair]
            other = sum(lax.dynamic_index_in_dim(term, 1 - bit, 1, keepdims=False) for term in split)
            mine = sum(lax.dynamic_index_in_dim(term, bit, 1, keepdims=False) for term in split)
            terms[at] = (mine, lax.ppermute(other, "ga", swap))
        span *= 2
    totals = [mine + other for mine, other in terms]
    results = [lax.dynamic_index_in_dim(total, place // span, 0, keepdims=False) for total in totals]
    rest = shards // span
    for step in range(1, rest):
        ring = [(s, (s + span * step) % shards) for s in range(shards)]
        for at, total in enumerate(totals):
            part = lax.dynamic_index_in_dim(total, (place // span + step) % rest, 0, keepdims=False)
            results[at] = results[at] + lax.ppermute(part, "ga", ring)
    return results


def local(coeffs, counts, block_map, wrap):
    held = coeffs[0]
    lines, g_rows, _, _ = held.shape
    shards = lax.axis_size("ga")
    per_shard = g_rows // BLK
    blocks = block_map.shape[-1]
    capacity = blocks // (shards * shards) + 1
    k_total = counts.shape[0]
    k = lax.axis_index("ka")
    g = lax.axis_index("ga")
    k_prev = (k + k_total - 1) % k_total
    ids = jnp.arange(per_shard, dtype=jnp.int32)
    slot_ids = jnp.arange(capacity, dtype=jnp.int32)
    shard_ids = jnp.arange(shards, dtype=jnp.int32)
    place = g.astype(jnp.int32).reshape(1)
    by_line = jnp.transpose(counts)
    down = [(s, (s - 1) % k_total) for s in range(k_total)]
    outs = []
    for line in range(lines):
        mine = lax.dynamic_slice_in_dim(block_map[k, line], g * per_shard, per_shard, 0)
        shift = lax.dynamic_slice_in_dim(wrap[k, line], g * per_shard, per_shard, 0)
        code = lax.optimization_barrier(((mine + 1) * BLK + shift) * per_shard + ids)
        target = (code // (per_shard * BLK) - 1) // per_shard
        earlier = ids[:, None] > ids[None, :]
        rank = jnp.sum(((target[:, None] == target[None, :]) & earlier).astype(jnp.int32), axis=1)
        left_rank = jnp.where(target[None, :] == shard_ids[:, None], rank[None, :], capacity)
        theirs = block_map[k_prev, line].reshape(shards, per_shard)
        for_me = theirs // per_shard == g
        rank_in = jnp.sum((for_me[:, None, :] & earlier[None]).astype(jnp.int32), axis=2)
        right_rank = jnp.where(for_me, rank_in, capacity)
        ranks = jnp.concatenate([left_rank, right_rank])
        values = jnp.concatenate([jnp.broadcast_to(code, (shards, per_shard)), theirs % per_shard])
        hit = ranks[:, None, :] == slot_ids[None, :, None]
        table = jnp.sum(jnp.where(hit, values[:, None, :], 0), axis=2).reshape(-1)

        rows = held[line]
        pieces = pieces_of(shards, capacity)
        lefts, rights = {}, {}
        for at, piece in enumerate(pieces):
            offset, first, end = piece
            jobs = [(piece, True), ((-offset, first, end), False)]

            def packed(chosen, table):
                made = pack(rows, table, place, by_line, chosen, capacity, shards, blocks, line)
                return lax.optimization_barrier((table, *made))

            if at < TOGETHER:
                table, left, right = packed(jobs, table)
            else:
                table, left = packed(jobs[:1], table)
            if offset:
                left = lax.ppermute(left, "ga", [(s, (s + offset) % shards) for s in range(shards)])
            if at >= TOGETHER:
                table, right = packed(jobs[1:], table)
            right = lax.ppermute(right, "ka", down)
            lefts[piece], rights[piece] = left, right
        groups = groups_of(pieces)
        total = None
        for group in groups:
            split = group is groups[-1]
            total = product([lefts[p] for p in group], [rights[p] for p in group], total, shards, split)
        outs.append(jnp.stack(scatter_sum(total[:2], total[2:], shards), axis=1))
    return jnp.stack(outs, axis=1)[None]


def solution(mesh):
    placed = (P("ka", None, "ga", None, None), P(), P(), P())

    return jax.shard_map(
        local,
        mesh=mesh,
        in_specs=placed,
        out_specs=P("ka", "ga", None, None, None),
        check_vma=False,
    )
```
